128 devices in a mesh: rows: 32 (over z, y, core), sub: 4 (over x).
Axes of the slice: x: 4, y: 4, z: 4, core: 2. Of those that a mesh axis runs over, the one named last changes fastest.
Arguments:
- snapshots: float32 [513, 131072], P(None, ('rows', 'sub')), may hold values from -6 to 6
- start: float32 [512, 64], replicated, may hold values from -6 to 6
Outputs:
- modes: float32 [128, 131072], P(None, ('rows', 'sub'))
- operator: float32 [128, 128], replicated
- coefficients: float32 [128, 513], replicated
The draws below stay inside these ranges and needn't reach their ends.
All inputs are finite; a program needn't handle non-finite values.
Results may differ from the reference program's by a relative error of at most 0.0003.
Values sent between devices are 32-bit elements; how exact they have to be, the bound alone decides.
A program may use at most 64 MiB of HBM per device.

```python
import jax
import jax.numpy as jnp
from jax import lax

SNAPS = 513
BLOCK = 64
STEPS = 2
RANK = 128
CELLS = 131072


def shard_levels(rng, shape, cuts, least, high):
    factor_of, own = 1.0, jax.random.fold_in(rng, 6)
    for position, blocks in cuts:
        steps = jnp.exp(jax.random.uniform(jax.random.fold_in(own, position), (blocks,), jnp.float32, least / len(cuts), high / len(cuts)))
        factor_of = factor_of * jnp.repeat(steps, shape[position] // blocks).reshape([-1 if axis == position else 1 for axis in range(len(shape))])
    return factor_of


def centred(rng, shape, scale, bound, cuts=(), kind=jnp.bfloat16):
    drawn = scale * jax.random.normal(rng, shape, jnp.float32)
    if cuts:
        drawn = drawn * shard_levels(rng, shape, cuts, -0.22, 0.18)
    return jnp.clip(drawn, -bound, bound).astype(kind)


def setup_inputs(seed: int = 0) -> dict:
    key_list = jax.random.split(jax.random.key(seed), 3)
    return {
        "snapshots": centred(key_list[0], (SNAPS, CELLS), 1.0, 6.0, ((1, 128),), jnp.float32),
        "start": centred(key_list[1], (SNAPS - 1, BLOCK), 1.0, 6.0, (), jnp.float32),
    }


def cross_cells(left, right):
    return lax.dot_general(left.astype(jnp.float32), right.astype(jnp.float32), (((1,), (1,)), ((), ())), precision=lax.Precision.HIGHEST, preferred_element_type=jnp.float32)

def matmul(left, right):
    return jnp.dot(left.astype(jnp.float32), right.astype(jnp.float32), precision=lax.Precision.HIGHEST, preferred_element_type=jnp.float32)

def factor_inverse(gram_block):
    factor = jnp.linalg.cholesky(gram_block)
    identity = jnp.eye(gram_block.shape[0], dtype=jnp.float32)
    inverse = jax.scipy.linalg.solve_triangular(factor, identity, lower=True)
    return (factor, inverse)

def orthonormal_columns(matrix):
    factor, inverse = factor_inverse(matmul(matrix.T, matrix))
    return matmul(matrix, inverse.T)

def reference(snapshots, start):
    width = start.shape[1]
    count = snapshots.shape[0]
    right_block = orthonormal_columns(start)
    right_blocks = [right_block]
    left_blocks = []
    columns = []
    for step in range(STEPS):
        padded = jnp.concatenate([right_block, jnp.zeros((1, width), jnp.float32)], 0)
        image = matmul(padded.T, snapshots)
        pieces = []
        if step > 0:
            earlier = jnp.concatenate(left_blocks, 0)
            coupling = cross_cells(earlier, image)
            image = image - matmul(coupling.T, earlier)
            pieces.append(coupling)
        factor, inverse = factor_inverse(cross_cells(image, image))
        left_blocks.append(matmul(inverse, image))
        pieces.append(factor.T)
        below = RANK - (step + 1) * width
        if below > 0:
            pieces.append(jnp.zeros((below, width), jnp.float32))
        columns.append(jnp.concatenate(pieces, 0))
        if step < STEPS - 1:
            back_sum = cross_cells(snapshots, left_blocks[-1])[:count - 1]
            basis = jnp.concatenate(right_blocks, 1)
            back_sum = back_sum - matmul(basis, matmul(basis.T, back_sum))
            right_block = orthonormal_columns(back_sum)
            right_blocks.append(right_block)
    triangle = jnp.concatenate(columns, 1)
    inverse_tri = jax.scipy.linalg.solve_triangular(triangle, jnp.eye(RANK, dtype=jnp.float32), lower=False)
    basis = jnp.concatenate(right_blocks, 1)
    shifted = jnp.concatenate([jnp.zeros((1, RANK), jnp.float32), basis], 0)
    advanced = matmul(shifted.T, snapshots)
    left_all = jnp.concatenate(left_blocks, 0)
    operator = matmul(cross_cells(left_all, advanced), inverse_tri)
    scale = jnp.sqrt(jnp.asarray(CELLS, jnp.float32))
    modes = scale * matmul(inverse_tri.T, advanced)
    mode_gram = cross_cells(modes, modes)
    mode_rhs = cross_cells(modes, snapshots)
    coefficients = jax.scipy.linalg.cho_solve((jnp.linalg.cholesky(mode_gram), True), mode_rhs)
    return (modes, operator, coefficients)
```

```python
import jax
import jax.numpy as jnp
from jax import lax
from jax.experimental import pallas as pl
from jax.experimental.pallas import tpu as pltpu
from jax.sharding import Mesh
from jax.sharding import PartitionSpec as P

ROWS_SUB = ("rows_0", "rows_1", "rows_2", "sub")
F32 = jnp.float32
BF16 = jnp.bfloat16
MESH = pl.DeviceIdType.MESH
HI = lax.Precision.HIGHEST
W = 64
PAST = 512
CELLS_HERE = 1024
BLOCKS = [(0, 0), (0, 1), (0, 2), (0, 3), (1, 1), (1, 2), (1, 3), (2, 2), (2, 3), (3, 3)]
TILES = 16 * len(BLOCKS)
HALF = TILES // 2
PIECE = HALF // 16


def dot_nn(a, b, precision=HI):
    return lax.dot_general(a, b, (((1,), (0,)), ((), ())), precision=precision, preferred_element_type=F32)


def dot_nt(a, b, precision=HI):
    return lax.dot_general(a, b, (((1,), (1,)), ((), ())), precision=precision, preferred_element_type=F32)


def dot_tn(a, b, precision=HI):
    return lax.dot_general(a, b, (((0,), (0,)), ((), ())), precision=precision, preferred_element_type=F32)


def iota(shape, dim):
    return lax.broadcasted_iota(jnp.int32, shape, dim)


def eliminate(mats):
    sub = iota((8, 128), 0)
    works = []
    eye = jnp.where(iota((W, W), 0) == iota((W, W), 1), 1.0, 0.0).astype(F32)
    for s in mats:
        aug = jnp.concatenate([s, eye], 1)
        works.append([aug[8 * i : 8 * i + 8] for i in range(8)])
    for k in range(8):
        for v in works:
            col = {}
            for i in range(k, 8):
                for q in range(8):
                    at = 8 * k + q
                    col[i, q] = jnp.broadcast_to(v[i][:, at : at + 1], (8, 128))
            scale = jnp.ones((8, 128), F32)
            for q in range(8):
                pivot = jnp.broadcast_to(col[k, q][q : q + 1], (8, 128))
                inv = lax.rsqrt(pivot)
                scale = jnp.where(sub == q, inv, scale)
                row = jnp.broadcast_to(v[k][q : q + 1], (8, 128)) * inv
                own = jnp.where(sub > q, col[k, q] * inv, 0.0)
                v[k] = v[k] - own * row
                low = {i: col[i, q] * inv for i in range(k + 1, 8)}
                for p in range(q + 1, 8):
                    at = jnp.broadcast_to(own[p : p + 1], (8, 128))
                    col[k, p] = col[k, p] - own * at
                    for i in low:
                        col[i, p] = col[i, p] - low[i] * at
                for i in low:
                    v[i] = v[i] - low[i] * row
            v[k] = v[k] * scale
    keep = iota((W, 128), 1) >= iota((W, 128), 0)
    return [jnp.where(keep, jnp.concatenate(v, 0), 0.0) for v in works]


def apply_u(fac, z):
    return dot_nn(fac, jnp.concatenate([z, jnp.zeros_like(z)], 0))


def apply_x(fac, z):
    return dot_nn(fac, jnp.concatenate([jnp.zeros_like(z), z], 0))


def apply_xt(fac, z):
    return dot_tn(fac, z)[W:]


def orth_kernel(start_ref, out_ref):
    start = start_ref[...]
    st = jnp.concatenate([start, jnp.zeros_like(start)], 1).T[:W]
    fac = eliminate([dot_nt(st, st)])[0]
    out_ref[...] = apply_x(fac, st)


def ring(axis, step):
    n = lax.axis_size(axis)
    return lax.rem(lax.axis_index(axis) + (step + n) % n, n)


def gram_kernel(x_ref, out_ref, hi, lo, part, mine, recv0, buf_a, buf_b, s0, r0, sa, ra, sb, rb, sg, rg, sd, rd):
    z, y, c, x = (lax.axis_index(a) for a in ROWS_SUB)
    offsets = [(o // 4, o % 4) for o in range(16)]

    def plane(o):
        return {"rows_1": ring("rows_1", offsets[o][0]), "sub": ring("sub", offsets[o][1])}

    def plane_source(o):
        return ring("rows_1", -offsets[o][0]) * 4 + ring("sub", -offsets[o][1])

    def plane_target(o):
        return ring("rows_1", offsets[o][0]) * 4 + ring("sub", offsets[o][1])

    barrier = pltpu.get_barrier_semaphore()
    partner = {"rows_2": 1 - c}
    pl.semaphore_signal(barrier, inc=1, device_id=partner, device_id_type=MESH)
    for o in range(1, 16):
        pl.semaphore_signal(barrier, inc=1, device_id=plane(o), device_id_type=MESH)
    for dz in range(1, 4):
        pl.semaphore_signal(barrier, inc=1, device_id={"rows_0": ring("rows_0", dz)}, device_id_type=MESH)

    last = jnp.broadcast_to(x_ref[PAST : PAST + 1], (16, CELLS_HERE))
    hl = last.astype(BF16)
    hi[0:16] = hl
    lo[0:16] = (last - hl.astype(F32)).astype(BF16)
    for r in range(0, PAST, 128):
        v = x_ref[r : r + 128]
        h = v.astype(BF16)
        hi[16 + r : 144 + r] = h
        lo[16 + r : 144 + r] = (v - h.astype(F32)).astype(BF16)
    lane = iota((8, 128), 1)
    row = iota((8, 128), 0)
    at = 0
    g = None
    for s in range(4):
        top = 0 if s == 0 else 16 + 128 * s
        rows = slice(top, 16 + 128 * (s + 1))
        cols = slice(16 + 128 * s, 16 + PAST)
        strip = dot_nt(hi[rows], hi[cols], None) + (dot_nt(hi[rows], lo[cols], None) + dot_nt(lo[rows], hi[cols], None))
        if s == 0:
            g = strip[0:8]
            strip = strip[16:]
            own = dot_nt(hi[0:16], hi[0:16], None) + (dot_nt(hi[0:16], lo[0:16], None) + dot_nt(lo[0:16], hi[0:16], None))
            corner = own[0:1, 0:1]
        for b in range(s, 4):
            block = strip[:, 128 * (b - s) : 128 * (b - s + 1)].reshape(16, 8, 128)
            part[at * 16 : at * 16 + 16] = block
            if b == s:
                gb = g[:, 128 * b : 128 * b + 128]
                packed = jnp.where(row == 0, gb, jnp.where(row == 1, pltpu.roll(gb, 64, 1), corner))
                part[at * 16 + 8] = jnp.where(lane < 64, packed, block[8])
            at += 1

    pl.semaphore_wait(barrier, 19)
    swap = pltpu.make_async_remote_copy(
        part.at[pl.ds((1 - c) * HALF, HALF)], recv0, s0, r0, device_id=partner, device_id_type=MESH
    )
    swap.start()
    swap.wait_recv()
    mine[...] = part[pl.ds(c * HALF, HALF)] + recv0[...]

    copies = []
    for o in range(15, 0, -1):
        copy = pltpu.make_async_remote_copy(
            mine.at[pl.ds(plane_target(o) * PIECE, PIECE)], buf_a.at[o], sa.at[o], ra.at[o], device_id=plane(o), device_id_type=MESH
        )
        copy.start()
        copies.append(copy)
    here = y * 4 + x
    total = mine[pl.ds(here * PIECE, PIECE)]
    for o in range(1, 16):
        copies[15 - o].wait_recv()
        total = total + buf_a[o]
    buf_b[z] = total
    for dz in range(1, 4):
        copy = pltpu.make_async_remote_copy(
            buf_b.at[z], buf_b.at[z], sb.at[dz], rb.at[dz], device_id={"rows_0": ring("rows_0", dz)}, device_id_type=MESH
        )
        copy.start()
        copies.append(copy)
    for dz in range(1, 4):
        copies[14 + dz].wait_recv()
    place = c * HALF + here * PIECE
    out_ref[pl.ds(place, PIECE)] = (buf_b[0] + buf_b[1]) + (buf_b[2] + buf_b[3])
    gathers = {}
    for o in range(15, 0, -1):
        copy = pltpu.make_async_remote_copy(
            out_ref.at[pl.ds(place, PIECE)],
            out_ref.at[pl.ds(place, PIECE)],
            sg.at[o],
            rg.at[o],
            device_id=plane(o),
            device_id_type=MESH,
        )
        copy.start()
        copies.append(copy)
        gathers[o] = copy
    forwards = []
    for o in range(16):
        if o:
            gathers[o].wait_recv()
        spot = pl.ds(c * HALF + plane_source(o) * PIECE, PIECE)
        copy = pltpu.make_async_remote_copy(
            out_ref.at[spot], out_ref.at[spot], sd.at[o], rd.at[o], device_id=partner, device_id_type=MESH
        )
        copy.start()
        forwards.append(copy)
    swap.wait_send()
    for copy in copies:
        copy.wait_send()
    for copy in forwards:
        copy.wait()


def gram(snapshots):
    dma = pltpu.SemaphoreType.DMA
    return pl.pallas_call(
        gram_kernel,
        out_shape=jax.ShapeDtypeStruct((TILES, 8, 128), F32),
        in_specs=[pl.BlockSpec(memory_space=pltpu.VMEM)],
        out_specs=pl.BlockSpec(memory_space=pltpu.VMEM),
        scratch_shapes=[
            pltpu.VMEM((16 + PAST, CELLS_HERE), BF16),
            pltpu.VMEM((16 + PAST, CELLS_HERE), BF16),
            pltpu.VMEM((TILES, 8, 128), F32),
            pltpu.VMEM((HALF, 8, 128), F32),
            pltpu.VMEM((HALF, 8, 128), F32),
            pltpu.VMEM((16, PIECE, 8, 128), F32),
            pltpu.VMEM((4, PIECE, 8, 128), F32),
            dma(()),
            dma(()),
            dma((16,)),
            dma((16,)),
            dma((4,)),
            dma((4,)),
            dma((16,)),
            dma((16,)),
            dma((16,)),
            dma((16,)),
        ],
        compiler_params=pltpu.CompilerParams(collective_id=0, has_side_effects=True),
        name="gram",
    )(snapshots)


def rest_kernel(tiles_ref, right_ref, x_hbm, modes_ref, operator_ref, coef_ref, gp, xv, sem, *, root):
    load = pltpu.make_async_copy(x_hbm, xv, sem)
    load.start()
    lane8 = iota((1, 128), 1)
    low_left = (iota((128, 128), 0) >= 64) & (iota((128, 128), 1) < 64)
    pieces, corner = [], None
    for n, (i, j) in enumerate(BLOCKS):
        block = tiles_ref[16 * n : 16 * n + 16].reshape(128, 128)
        if i == j:
            extra = block[64:72]
            pieces.append(jnp.where(lane8 < 64, extra[0:1], pltpu.roll(extra[1:2], 64, 1)))
            if corner is None:
                corner = extra[2:3, 0:1]
            block = jnp.where(low_left, block.T, block)
        else:
            gp[128 * j : 128 * j + 128, 128 * i : 128 * i + 128] = block.T
        gp[128 * i : 128 * i + 128, 128 * j : 128 * j + 128] = block
    g = jnp.concatenate(pieces, 1)
    first = iota((W, PAST), 1) == 0

    def products(vt):
        around = pltpu.roll(vt, 1, 1)
        shifted = jnp.where(first, 0.0, around)
        end = vt[:, PAST - 1 : PAST]
        both = dot_nn(jnp.concatenate([vt, shifted], 0), gp[...])
        q = both[W:] + end * g
        q_end = jnp.sum(shifted * g, 1, keepdims=True) + end * corner
        q_around = jnp.where(first, q_end, q)
        q_wide = jnp.concatenate([q, jnp.where(iota((W, 128), 1) == 0, q_end, 0.0)], 1)
        return both[:W], around, q_around, q_wide

    v1 = right_ref[...]
    a, v1c, q1c, q1 = products(v1)
    m1 = dot_nt(a, v1)
    c11 = dot_nt(q1c, v1c)
    e = a - dot_nn(m1, v1)
    eye = iota((W, W), 0) == iota((W, W), 1)
    e = e / jnp.sum(jnp.where(eye, m1, 0.0), 1, keepdims=True)
    f1, fc1 = eliminate([m1, c11])
    b, ec, q2c, q2 = products(e)
    h12 = dot_nt(a, e)
    h22 = dot_nt(b, e)
    c12 = dot_nt(q1c, ec)
    c22 = dot_nt(q2c, ec)
    u12 = apply_x(f1, h12)
    uc12 = apply_x(fc1, c12)
    f2, fc2 = eliminate([h22 - dot_tn(u12, u12), c22 - dot_tn(uc12, uc12)])

    w1 = apply_x(f1, jnp.concatenate([v1, v1c, q1], 1))
    y2 = jnp.concatenate([e, ec, q2], 1) - dot_tn(u12, w1)
    w2 = apply_x(f2, y2)
    wt = jnp.concatenate([w1[:, :PAST], w2[:, :PAST]], 0)
    qw = jnp.concatenate([w1[:, 2 * PAST : 3 * PAST], w2[:, 2 * PAST : 3 * PAST]], 0)
    operator_ref[...] = dot_nt(wt, qw)

    t1 = apply_x(fc1, q1)
    y_2 = apply_xt(fc2, apply_x(fc2, q2 - dot_tn(uc12, t1)))
    y_1 = apply_xt(fc1, t1 - dot_nn(uc12, y_2))
    top = apply_u(f1, y_1) + dot_nn(u12, y_2)
    coef = jnp.concatenate([top, apply_u(f2, y_2)], 0) * (1.0 / root)
    coef_ref[:, :PAST] = coef[:, :PAST]
    coef_ref[:, PAST : PAST + 1] = coef[:, PAST : PAST + 1]

    load.wait()
    xv[0:1] = xv[PAST : PAST + 1]
    wc = jnp.concatenate([w1[:, PAST : 2 * PAST], w2[:, PAST : 2 * PAST]], 0) * root
    modes_ref[...] = dot_nn(wc, xv[0:PAST], lax.Precision.HIGH)


def rest(tiles, right, snapshots, cells):
    vm = pl.BlockSpec(memory_space=pltpu.VMEM)
    order = 2 * W
    return pl.pallas_call(
        lambda *refs: rest_kernel(*refs, root=float(cells) ** 0.5),
        out_shape=[
            jax.ShapeDtypeStruct((order, CELLS_HERE), F32),
            jax.ShapeDtypeStruct((order, order), F32),
            jax.ShapeDtypeStruct((order, PAST + 1), F32),
        ],
        in_specs=[vm, vm, pl.BlockSpec(memory_space=pl.ANY)],
        out_specs=[vm, vm, vm],
        scratch_shapes=[
            pltpu.VMEM((PAST, PAST), F32),
            pltpu.VMEM((PAST + 1, CELLS_HERE), F32),
            pltpu.SemaphoreType.DMA(()),
        ],
        compiler_params=pltpu.CompilerParams(vmem_limit_bytes=40 * 1024 * 1024),
        name="rest",
    )(tiles, right, snapshots)


def orth(start):
    vm = pl.BlockSpec(memory_space=pltpu.VMEM)
    return pl.pallas_call(
        orth_kernel, out_shape=jax.ShapeDtypeStruct((W, PAST), F32), in_specs=[vm], out_specs=vm, name="orth"
    )(start)


def shards(snapshots, start):
    cells = snapshots.shape[1] * lax.axis_size(ROWS_SUB)
    right = orth(start)
    tiles = gram(snapshots)
    return tuple(rest(tiles, right, snapshots, cells))


def solution(mesh):
    finer = Mesh(mesh.devices.reshape(4, 4, 2, mesh.shape["sub"]), ROWS_SUB)
    return jax.shard_map(
        shards,
        mesh=finer,
        in_specs=(P(None, ROWS_SUB), P()),
        out_specs=(P(None, ROWS_SUB), P(), P()),
        check_vma=False,
    )
```

```python
import jax
import jax.numpy as jnp
from jax import lax
from jax.experimental import pallas as pl
from jax.experimental.pallas import tpu as pltpu
from jax.sharding import Mesh
from jax.sharding import PartitionSpec as P

ROWS_SUB = ("rows_0", "rows_1", "rows_2", "sub")
F32 = jnp.float32
BF16 = jnp.bfloat16
MESH = pl.DeviceIdType.MESH
HI = lax.Precision.HIGHEST
W = 64
PAST = 512
CELLS_HERE = 1024
BLOCKS = [(0, 0), (0, 1), (0, 2), (2, 2), (2, 3)] + [(1, 1), (1, 2), (1, 3), (3, 3), (3, 0)]
TILES = 16 * len(BLOCKS)
HALF = TILES // 2
PIECE = HALF // 16
CHUNKS = 2
DEPTH = CELLS_HERE // CHUNKS
GRANT = 24


def dot_nn(a, b, precision=HI):
    return lax.dot_general(a, b, (((1,), (0,)), ((), ())), precision=precision, preferred_element_type=F32)


def dot_nt(a, b, precision=HI):
    return lax.dot_general(a, b, (((1,), (1,)), ((), ())), precision=precision, preferred_element_type=F32)


def dot_tn(a, b, precision=HI):
    return lax.dot_general(a, b, (((0,), (0,)), ((), ())), precision=precision, preferred_element_type=F32)


def iota(shape, dim):
    return lax.broadcasted_iota(jnp.int32, shape, dim)


def eliminate(mats):
    sub = iota((8, 128), 0)
    works = []
    eye = jnp.where(iota((W, W), 0) == iota((W, W), 1), 1.0, 0.0).astype(F32)
    for s in mats:
        aug = jnp.concatenate([s, eye], 1)
        works.append([aug[8 * i : 8 * i + 8] for i in range(8)])
    for k in range(8):
        for v in works:
            col = {}
            for i in range(k, 8):
                for q in range(8):
                    at = 8 * k + q
                    col[i, q] = jnp.broadcast_to(v[i][:, at : at + 1], (8, 128))
            scale = jnp.ones((8, 128), F32)
            for q in range(8):
                pivot = jnp.broadcast_to(col[k, q][q : q + 1], (8, 128))
                inv = lax.rsqrt(pivot)
                scale = jnp.where(sub == q, inv, scale)
                row = jnp.broadcast_to(v[k][q : q + 1], (8, 128)) * inv
                own = jnp.where(sub > q, col[k, q] * inv, 0.0)
                v[k] = v[k] - own * row
                low = {i: col[i, q] * inv for i in range(k + 1, 8)}
                for p in range(q + 1, 8):
                    at = jnp.broadcast_to(own[p : p + 1], (8, 128))
                    col[k, p] = col[k, p] - own * at
                    for i in low:
                        col[i, p] = col[i, p] - low[i] * at
                for i in low:
                    v[i] = v[i] - low[i] * row
            v[k] = v[k] * scale
    keep = iota((W, 128), 1) >= iota((W, 128), 0)
    return [jnp.where(keep, jnp.concatenate(v, 0), 0.0) for v in works]


def apply_u(fac, z):
    return dot_nn(fac, jnp.concatenate([z, jnp.zeros_like(z)], 0))


def apply_x(fac, z):
    return dot_nn(fac, jnp.concatenate([jnp.zeros_like(z), z], 0))


def apply_xt(fac, z):
    return dot_tn(fac, z)[W:]


def orth_rows(st):
    return apply_x(eliminate([dot_nt(st, st)])[0], st)


def ring(axis, step):
    n = lax.axis_size(axis)
    return lax.rem(lax.axis_index(axis) + (step + n) % n, n)


def gram_kernel(
    x_hbm, start_hbm, out_ref, right_ref, xv, sv, hi, lo, hx, lx, part, mine, recv0, buf_a, buf_b, sx, ss, s0, r0, sa, ra, sb, rb, sg, rg, sd, rd
):
    loads = []
    for t in range(CHUNKS):
        cols = pl.ds(t * DEPTH, DEPTH)
        loads.append(pltpu.make_async_copy(x_hbm.at[:, cols], xv.at[:, cols], sx.at[t]))
        loads[-1].start()
    start_load = pltpu.make_async_copy(start_hbm, sv, ss)
    start_load.start()
    z, y, c, x = (lax.axis_index(a) for a in ROWS_SUB)
    offsets = [(o // 4, o % 4) for o in range(16)]
    hops = [min(dy, 4 - dy) + min(dx, 4 - dx) for dy, dx in offsets]
    near_first = sorted(range(1, 16), key=lambda o: hops[o])

    def plane(o):
        return {"rows_1": ring("rows_1", offsets[o][0]), "sub": ring("sub", offsets[o][1])}

    def plane_source(o):
        return ring("rows_1", -offsets[o][0]) * 4 + ring("sub", -offsets[o][1])

    def plane_target(o):
        return ring("rows_1", offsets[o][0]) * 4 + ring("sub", offsets[o][1])

    barrier = pltpu.get_barrier_semaphore()
    partner = {"rows_2": 1 - c}
    for o in near_first[::-1]:
        pl.semaphore_signal(barrier, inc=1, device_id=plane(o), device_id_type=MESH)
    for dz in range(1, 4):
        pl.semaphore_signal(barrier, inc=1, device_id={"rows_0": ring("rows_0", dz)}, device_id_type=MESH)
    pl.semaphore_signal(barrier, inc=1, device_id=partner, device_id_type=MESH)

    lane = iota((8, 128), 1)
    row = iota((8, 128), 0)
    own_g = {}
    corner = jnp.zeros((1, 1), F32)
    swap = pltpu.make_async_remote_copy(
        part.at[pl.ds((1 - c) * HALF, HALF)], recv0, s0, r0, device_id=partner, device_id_type=MESH
    )
    for t in range(CHUNKS):
        k = slice(t * DEPTH, (t + 1) * DEPTH)
        loads[t].wait()
        last = xv[PAST : PAST + 1, k]
        corner = corner + jnp.sum(last * last, 1, keepdims=True)
        last = jnp.broadcast_to(last, (16, DEPTH))
        hl = last.astype(BF16)
        hx[:, k] = hl
        lx[:, k] = (last - hl.astype(F32)).astype(BF16)
        for r in range(0, PAST, 128):
            v = xv[r : r + 128, k]
            h = v.astype(BF16)
            low = (v - h.astype(F32)).astype(BF16)
            hi[r : r + 128, k] = h
            lo[r : r + 128, k] = low
            if r == 0:
                hi[PAST : PAST + 128, k] = h
                lo[PAST : PAST + 128, k] = low
        for own in range(2):
            p = c if own else 1 - c
            for s in range(2):
                first = pl.multiple_of((p + 2 * s) * 128, 128)
                width = 384 - 128 * s
                lines, across = pl.ds(first, 128), pl.ds(first, width)
                a = jnp.concatenate([hx[:, k], hi[lines, k]], 0)
                b = jnp.concatenate([lx[:, k], lo[lines, k]], 0)
                strip = dot_nt(a, hi[across, k], None) + (dot_nt(a, lo[across, k], None) + dot_nt(b, hi[across, k], None))
                gs = strip[0:8, 0:128]
                if t:
                    gs = gs + own_g[own, s]
                own_g[own, s] = gs
                for n in range(width // 128):
                    spot = p * HALF + 16 * (3 * s + n)
                    block = strip[16:, 128 * n : 128 * n + 128].reshape(16, 8, 128)
                    if t:
                        block = block + part[pl.ds(spot, 16)]
                    part[pl.ds(spot, 16)] = block
                    if n == 0 and t == CHUNKS - 1:
                        packed = jnp.where(row == 0, gs, jnp.where(row == 1, pltpu.roll(gs, 64, 1), corner))
                        part[spot + 8] = jnp.where(lane < 64, packed, block[8])
            if t == CHUNKS - 1 and own == 0:
                pl.semaphore_wait(barrier, 19)
                swap.start()

    swap.wait_recv()
    mine[...] = part[pl.ds(c * HALF, HALF)] + recv0[...]

    copies = []
    arrivals = {}
    for o in near_first[::-1]:
        arrivals[o] = pltpu.make_async_remote_copy(
            mine.at[pl.ds(plane_target(o) * PIECE, PIECE)], buf_a.at[o], sa.at[o], ra.at[o], device_id=plane(o), device_id_type=MESH
        )
        arrivals[o].start()
        copies.append(arrivals[o])
    start_load.wait()
    right_ref[...] = orth_rows(sv[...])
    here = y * 4 + x
    total = mine[pl.ds(here * PIECE, PIECE)]
    for o in near_first:
        arrivals[o].wait_recv()
        total = total + buf_a[o]
    buf_b[z] = total
    for dz in range(1, 4):
        copy = pltpu.make_async_remote_copy(
            buf_b.at[z], buf_b.at[z], sb.at[dz], rb.at[dz], device_id={"rows_0": ring("rows_0", dz)}, device_id_type=MESH
        )
        copy.start()
        copies.append(copy)
    for copy in copies[-3:]:
        copy.wait_recv()
    place = c * HALF + here * PIECE
    out_ref[pl.ds(place, PIECE)] = (buf_b[0] + buf_b[1]) + (buf_b[2] + buf_b[3])
    gathers = {}
    for o in near_first[::-1]:
        spot = pl.ds(place, PIECE)
        gathers[o] = pltpu.make_async_remote_copy(
            out_ref.at[spot], out_ref.at[spot], sg.at[o], rg.at[o], device_id=plane(o), device_id_type=MESH
        )
        gathers[o].start()
        copies.append(gathers[o])
    forwards = []
    for o in [0] + near_first:
        if o:
            gathers[o].wait_recv()
        spot = pl.ds(c * HALF + plane_source(o) * PIECE, PIECE)
        copy = pltpu.make_async_remote_copy(
            out_ref.at[spot], out_ref.at[spot], sd.at[o], rd.at[o], device_id=partner, device_id_type=MESH
        )
        copy.start()
        forwards.append(copy)
    swap.wait_send()
    for copy in copies:
        copy.wait_send()
    for copy in forwards:
        copy.wait()


def gram(snapshots, start_rows):
    dma = pltpu.SemaphoreType.DMA
    vm = pl.BlockSpec(memory_space=pltpu.VMEM)
    return pl.pallas_call(
        gram_kernel,
        out_shape=[jax.ShapeDtypeStruct((TILES, 8, 128), F32), jax.ShapeDtypeStruct((W, PAST), F32)],
        in_specs=[pl.BlockSpec(memory_space=pltpu.HBM)] * 2,
        out_specs=[vm, vm],
        scratch_shapes=[
            pltpu.VMEM((PAST + 1, CELLS_HERE), F32),
            pltpu.VMEM((W, PAST), F32),
            pltpu.VMEM((PAST + 128, CELLS_HERE), BF16),
            pltpu.VMEM((PAST + 128, CELLS_HERE), BF16),
            pltpu.VMEM((16, CELLS_HERE), BF16),
            pltpu.VMEM((16, CELLS_HERE), BF16),
            pltpu.VMEM((TILES, 8, 128), F32),
            pltpu.VMEM((HALF, 8, 128), F32),
            pltpu.VMEM((HALF, 8, 128), F32),
            pltpu.VMEM((16, PIECE, 8, 128), F32),
            pltpu.VMEM((4, PIECE, 8, 128), F32),
            dma((CHUNKS,)),
            dma(()),
            dma(()),
            dma(()),
            dma((16,)),
            dma((16,)),
            dma((4,)),
            dma((4,)),
            dma((16,)),
            dma((16,)),
            dma((16,)),
            dma((16,)),
        ],
        compiler_params=pltpu.CompilerParams(
            collective_id=0, has_side_effects=True, vmem_limit_bytes=GRANT * 1024 * 1024
        ),
        name="gram",
    )(snapshots, start_rows)


def rest_kernel(tiles_ref, right_ref, x_hbm, modes_ref, operator_ref, coef_ref, gp, xv, sem, *, root):
    load = pltpu.make_async_copy(x_hbm, xv, sem)
    load.start()
    lane8 = iota((1, 128), 1)
    low_left = (iota((128, 128), 0) >= 64) & (iota((128, 128), 1) < 64)
    pieces, corner = {}, None
    for n, (i, j) in enumerate(BLOCKS):
        block = tiles_ref[16 * n : 16 * n + 16].reshape(128, 128)
        if i == j:
            extra = block[64:72]
            pieces[i] = jnp.where(lane8 < 64, extra[0:1], pltpu.roll(extra[1:2], 64, 1))
            if corner is None:
                corner = extra[2:3, 0:1]
            block = jnp.where(low_left, block.T, block)
        else:
            gp[128 * j : 128 * j + 128, 128 * i : 128 * i + 128] = block.T
        gp[128 * i : 128 * i + 128, 128 * j : 128 * j + 128] = block
    g = jnp.concatenate([pieces[i] for i in range(4)], 1)
    first = iota((W, PAST), 1) == 0

    def products(vt):
        around = pltpu.roll(vt, 1, 1)
        shifted = jnp.where(first, 0.0, around)
        end = vt[:, PAST - 1 : PAST]
        both = dot_nn(jnp.concatenate([vt, shifted], 0), gp[...])
        q = both[W:] + end * g
        q_end = jnp.sum(shifted * g, 1, keepdims=True) + end * corner
        q_around = jnp.where(first, q_end, q)
        q_wide = jnp.concatenate([q, jnp.where(iota((W, 128), 1) == 0, q_end, 0.0)], 1)
        return both[:W], around, q_around, q_wide

    v1 = right_ref[...]
    a, v1c, q1c, q1 = products(v1)
    m1 = dot_nt(a, v1)
    c11 = dot_nt(q1c, v1c)
    e = a - dot_nn(m1, v1)
    eye = iota((W, W), 0) == iota((W, W), 1)
    e = e / jnp.sum(jnp.where(eye, m1, 0.0), 1, keepdims=True)
    f1, fc1 = eliminate([m1, c11])
    b, ec, q2c, q2 = products(e)
    h12 = dot_nt(a, e)
    h22 = dot_nt(b, e)
    c12 = dot_nt(q1c, ec)
    c22 = dot_nt(q2c, ec)
    u12 = apply_x(f1, h12)
    uc12 = apply_x(fc1, c12)
    f2, fc2 = eliminate([h22 - dot_tn(u12, u12), c22 - dot_tn(uc12, uc12)])

    w1 = apply_x(f1, jnp.concatenate([v1, v1c, q1], 1))
    y2 = jnp.concatenate([e, ec, q2], 1) - dot_tn(u12, w1)
    w2 = apply_x(f2, y2)
    wt = jnp.concatenate([w1[:, :PAST], w2[:, :PAST]], 0)
    qw = jnp.concatenate([w1[:, 2 * PAST : 3 * PAST], w2[:, 2 * PAST : 3 * PAST]], 0)
    operator_ref[...] = dot_nt(wt, qw)

    t1 = apply_x(fc1, q1)
    y_2 = apply_xt(fc2, apply_x(fc2, q2 - dot_tn(uc12, t1)))
    y_1 = apply_xt(fc1, t1 - dot_nn(uc12, y_2))
    top = apply_u(f1, y_1) + dot_nn(u12, y_2)
    coef = jnp.concatenate([top, apply_u(f2, y_2)], 0) * (1.0 / root)
    coef_ref[...] = coef.T[: PAST + 1]

    load.wait()
    xv[0:1] = xv[PAST : PAST + 1]
    wc = jnp.concatenate([w1[:, PAST : 2 * PAST], w2[:, PAST : 2 * PAST]], 0) * root
    modes_ref[...] = dot_nn(wc, xv[0:PAST], lax.Precision.HIGH)


def rest(tiles, right, snapshots, cells):
    vm = pl.BlockSpec(memory_space=pltpu.VMEM)
    order = 2 * W
    return pl.pallas_call(
        lambda *refs: rest_kernel(*refs, root=float(cells) ** 0.5),
        out_shape=[
            jax.ShapeDtypeStruct((order, CELLS_HERE), F32),
            jax.ShapeDtypeStruct((order, order), F32),
            jax.ShapeDtypeStruct((PAST + 1, order), F32),
        ],
        in_specs=[vm, vm, pl.BlockSpec(memory_space=pltpu.HBM)],
        out_specs=[vm, vm, vm],
        scratch_shapes=[
            pltpu.VMEM((PAST, PAST), F32),
            pltpu.VMEM((PAST + 1, CELLS_HERE), F32),
            pltpu.SemaphoreType.DMA(()),
        ],
        compiler_params=pltpu.CompilerParams(vmem_limit_bytes=GRANT * 1024 * 1024),
        name="rest",
    )(tiles, right, snapshots)


def shards(snapshots, start):
    cells = snapshots.shape[1] * lax.axis_size(ROWS_SUB)
    snapshots = pltpu.with_memory_space_constraint(snapshots, pltpu.HBM)
    tiles, right = gram(snapshots, pltpu.with_memory_space_constraint(start.T, pltpu.HBM))
    modes, operator, coef = rest(tiles, right, snapshots, cells)
    return modes, operator, coef.T


def solution(mesh):
    finer = Mesh(mesh.devices.reshape(4, 4, 2, mesh.shape["sub"]), ROWS_SUB)
    return jax.shard_map(
        shards,
        mesh=finer,
        in_specs=(P(None, ROWS_SUB), P()),
        out_specs=(P(None, ROWS_SUB), P(), P()),
        check_vma=False,
    )
```
